32 devices in a mesh: tm: 4 (over x, core), space: 8 (over z, y).
Axes of the slice: x: 2, y: 2, z: 4, core: 2. Of those that a mesh axis runs over, the one named last changes fastest.
Arguments:
- iterate: float32 [64, 16, 3, 4096], P('space', 'tm'), may hold values from -6 to 6
- forcing: float32 [64, 16, 3, 4096], P('space', 'tm'), may hold values from -6 to 6
- initial_velocity: float32 [64, 3, 4096], P('space'), may hold values from -6 to 6
- viscosity: float32 [64, 4096], P('space'), may hold values from 0.1 to 1
- peclet: float32 [64, 3, 4096], P('space'), may hold values from -0.9 to 0.9
- live_patch_mask: int32 [64], P('space'), may hold values from 0 to 1, as said below
- neighbour_holder: int32 [64, 6], P('space'), may hold values from -1 to 7, as said below
- neighbour_slot: int32 [64, 6], P('space'), may hold values from -1 to 7, as said below
Outputs:
- corrected_velocity: float32 [64, 16, 3, 4096], P('space', 'tm')
- corrected_residual: float32 [64, 16, 3, 4096], P('space', 'tm')
The draws below stay inside these ranges and needn't reach their ends.
Inputs may be any that keep to these rules, and one draw needn't show every extreme that they name: `live_patch_mask`: on each index of space the live slots (1) come first; their count is 2 to 8, and in every draw some two indices j and j + 4 have all 8 slots live. `neighbour_holder`: the patches of one index s of space are the blocks of one aligned 2x2x2 octant; the octant's position is read from the bits of s: bit b of s is bit b div 3 of coordinate b mod 3, except that where a coordinate has two bits its lower bit is complemented when its higher bit is 1; slot p lies at offsets (p mod 2, p div 2 mod 2, p div 4); the entry is -1 where no live patch lies across the face or the slot is dead; the relation is symmetric across opposite faces; the live patches of one index face those of another given index across at most 4 faces, exactly 4 for some pair in every draw. `neighbour_slot`: -1 exactly where neighbour_holder is -1.
All inputs are finite; a program needn't handle non-finite values.
Results may differ from the reference program's by a relative error of at most 0.0003.
Values sent between devices are 32-bit elements; how exact they have to be, the bound alone decides.
A program may use at most 192 MiB of HBM per device.

```python
import math
from functools import partial
import jax
import jax.numpy as jnp
from jax import lax

WINDOW_SLICES = 16
BLOCK_EDGE = 16
SLOTS_PER_SPACE = 8
SWEEPS = 5
TOTAL_SLOTS = 64
BLOCK_CELLS = 4096


def octant_layout(key):
    key = jax.random.fold_in(key, 7919)
    count_key, pair_key = jax.random.split(key)
    space_members = TOTAL_SLOTS // SLOTS_PER_SPACE
    levels = max(space_members - 1, 1).bit_length()
    half_members = max(space_members // 2, 1)
    counts = jax.random.randint(count_key, (space_members,), 2, 7)
    chosen = jax.random.randint(pair_key, (), 0, half_members)
    if space_members >= 16:
        chosen = jnp.bitwise_or(chosen, 1)
    device_ids = jnp.arange(space_members, dtype=jnp.int32)
    counts = jnp.where(device_ids % half_members == chosen, SLOTS_PER_SPACE, counts).astype(jnp.int32)
    slot_numbers = jnp.arange(TOTAL_SLOTS, dtype=jnp.int32)
    holders = slot_numbers // SLOTS_PER_SPACE
    local_slot = slot_numbers % SLOTS_PER_SPACE
    octant = [jnp.zeros_like(slot_numbers), jnp.zeros_like(slot_numbers), jnp.zeros_like(slot_numbers)]
    extents = [2, 2, 2]
    coord_bits = [0, 0, 0]
    for bit_index in range(levels):
        octant[bit_index % 3] = octant[bit_index % 3] + ((holders >> bit_index & 1) << bit_index // 3)
        extents[bit_index % 3] = extents[bit_index % 3] * 2
        coord_bits[bit_index % 3] = coord_bits[bit_index % 3] + 1
    for axis_id in range(3):
        if coord_bits[axis_id] == 2:
            octant[axis_id] = jnp.bitwise_xor(octant[axis_id], octant[axis_id] >> 1 & 1)
    coords = [2 * octant[axis_id] + (local_slot >> axis_id & 1) for axis_id in range(3)]
    live_self = local_slot < counts[holders]
    owner_columns = []
    slot_columns = []
    for face_id in range(6):
        axis_id = face_id // 2
        shifted = list(coords)
        shifted[axis_id] = coords[axis_id] + (2 * (face_id % 2) - 1)
        inside = (shifted[axis_id] >= 0) & (shifted[axis_id] < extents[axis_id])
        clipped = [jnp.clip(shifted[other_axis], 0, extents[other_axis] - 1) for other_axis in range(3)]
        decoded = []
        for other_axis in range(3):
            value = clipped[other_axis] // 2
            if coord_bits[other_axis] == 2:
                value = jnp.bitwise_xor(value, value >> 1 & 1)
            decoded.append(value)
        octant_code = jnp.zeros_like(slot_numbers)
        for bit_index in range(levels):
            octant_code = octant_code + ((decoded[bit_index % 3] >> bit_index // 3 & 1) << bit_index)
        neighbour_local = (clipped[0] & 1) + ((clipped[1] & 1) << 1) + ((clipped[2] & 1) << 2)
        in_range = octant_code < space_members
        safe_code = jnp.minimum(octant_code, space_members - 1)
        present = inside & in_range & live_self & (neighbour_local < counts[safe_code])
        owner_columns.append(jnp.where(present, octant_code, -1))
        slot_columns.append(jnp.where(present, neighbour_local, -1))
    live_mask = live_self.astype(jnp.int32)
    return (live_mask, jnp.stack(owner_columns, axis=1).astype(jnp.int32), jnp.stack(slot_columns, axis=1).astype(jnp.int32))


def draw_live_patch_mask(key, part):
    return octant_layout(key)[0]


def draw_neighbour_holder(key, part):
    return octant_layout(key)[1]


def draw_neighbour_slot(key, part):
    return octant_layout(key)[2]


def steps_of(rng, shape, cuts, low, largest):
    level = 1.0
    for dim, parts in cuts:
        draws = jax.random.uniform(jax.random.fold_in(jax.random.fold_in(rng, 6), dim), (parts,), jnp.float32, low / len(cuts), largest / len(cuts))
        level = level * jnp.repeat(jnp.exp(draws), shape[dim] // parts).reshape((-1,) + (1,) * (len(shape) - 1 - dim))
    return level


def centred(stream_key, dims, scale, limit, cuts=(), kind=jnp.bfloat16):
    result = jax.random.normal(stream_key, dims, jnp.float32) * scale
    if len(cuts) > 0:
        result = steps_of(stream_key, dims, cuts, -0.22, 0.18) * result
    return jnp.clip(result, min=-limit, max=limit).astype(kind)


def setup_inputs(seed: int = 0) -> dict:
    seeds = jax.random.split(jax.random.key(seed), 9)
    return {
        "iterate": centred(seeds[0], (TOTAL_SLOTS, WINDOW_SLICES, 3, BLOCK_CELLS), 1.0, 6.0, ((0, 8), (1, 4)), jnp.float32),
        "forcing": centred(seeds[1], (TOTAL_SLOTS, WINDOW_SLICES, 3, BLOCK_CELLS), 1.0, 6.0, ((0, 8), (1, 4)), jnp.float32),
        "initial_velocity": centred(seeds[2], (TOTAL_SLOTS, 3, BLOCK_CELLS), 1.0, 6.0, ((0, 8),), jnp.float32),
        "viscosity": jnp.clip(jnp.exp(math.log(1.0) - 2.3025851 * jax.random.uniform(seeds[3], (TOTAL_SLOTS, BLOCK_CELLS), jnp.float32) ** steps_of(seeds[3], (TOTAL_SLOTS, BLOCK_CELLS), ((0, 8),), -0.2, 0.2)), 0.1, 1.0),
        "peclet": jnp.clip(jax.random.uniform(seeds[4], (TOTAL_SLOTS, 3, BLOCK_CELLS), jnp.float32, -0.9, 0.9) * steps_of(seeds[4], (TOTAL_SLOTS, 3, BLOCK_CELLS), ((0, 8),), -0.4, 0.0), -0.9, 0.9),
        "live_patch_mask": draw_live_patch_mask(jax.random.fold_in(seeds[8], 71), 0),
        "neighbour_holder": draw_neighbour_holder(jax.random.fold_in(seeds[8], 71), 0),
        "neighbour_slot": draw_neighbour_slot(jax.random.fold_in(seeds[8], 71), 0),
    }


STEP_DURATION = 0.5
ALPHA_SCALE = 0.1
HIGHEST_PRECISION = lax.Precision.HIGHEST


def face_layers(block_shaped):
    return jnp.stack([block_shaped[:, :, 0], block_shaped[:, :, -1], block_shaped[:, :, :, 0], block_shaped[:, :, :, -1], block_shaped[:, :, :, :, 0], block_shaped[:, :, :, :, -1]], axis=1)


def across_faces(block_shaped, neighbour_holder, neighbour_slot):
    patch_count = block_shaped.shape[0]
    channels = block_shaped.shape[1]
    layers = face_layers(block_shaped).reshape(patch_count * 6, channels, BLOCK_EDGE, BLOCK_EDGE)
    opposite = jnp.array([1, 0, 3, 2, 5, 4], dtype=jnp.int32)
    source = (jnp.maximum(neighbour_holder, 0) * SLOTS_PER_SPACE + jnp.maximum(neighbour_slot, 0)) * 6 + opposite[None, :]
    gathered = jnp.take(layers, source.reshape(-1).astype(jnp.int32), axis=0).reshape(patch_count, 6, channels, BLOCK_EDGE, BLOCK_EDGE)
    present = (neighbour_holder >= 0) & (neighbour_slot >= 0)
    return jnp.where(present[:, :, None, None, None], gathered, jnp.zeros_like(gathered))


def adjacent_total(block_shaped, ghost_faces, peclet_shaped):
    padded = jnp.pad(block_shaped, ((0, 0), (0, 0), (1, 1), (1, 1), (1, 1)))
    padded = padded.at[:, :, 0, 1:-1, 1:-1].set(ghost_faces[:, 0])
    padded = padded.at[:, :, -1, 1:-1, 1:-1].set(ghost_faces[:, 1])
    padded = padded.at[:, :, 1:-1, 0, 1:-1].set(ghost_faces[:, 2])
    padded = padded.at[:, :, 1:-1, -1, 1:-1].set(ghost_faces[:, 3])
    padded = padded.at[:, :, 1:-1, 1:-1, 0].set(ghost_faces[:, 4])
    padded = padded.at[:, :, 1:-1, 1:-1, -1].set(ghost_faces[:, 5])
    x_peclet = peclet_shaped[:, 0:1]
    y_peclet = peclet_shaped[:, 1:2]
    z_peclet = peclet_shaped[:, 2:3]
    summed = (1.0 - x_peclet) * padded[:, :, 2:, 1:-1, 1:-1] + (1.0 + x_peclet) * padded[:, :, :-2, 1:-1, 1:-1]
    summed = summed + (1.0 - y_peclet) * padded[:, :, 1:-1, 2:, 1:-1] + (1.0 + y_peclet) * padded[:, :, 1:-1, :-2, 1:-1]
    summed = summed + (1.0 - z_peclet) * padded[:, :, 1:-1, 1:-1, 2:] + (1.0 + z_peclet) * padded[:, :, 1:-1, 1:-1, :-2]
    return summed


def residual_grid(velocity_state, forcing_history, initial_velocity, viscosity, peclet_shaped, live_indicator, neighbour_holder, neighbour_slot):
    earlier = jnp.concatenate([initial_velocity[None], velocity_state[:-1]], axis=0)

    def one_slice(pieces):
        present_iterate, prior_velocity, right_hand_side = pieces
        block_shaped = present_iterate.reshape(TOTAL_SLOTS, 3, BLOCK_EDGE, BLOCK_EDGE, BLOCK_EDGE)
        ghost_faces = across_faces(block_shaped, neighbour_holder, neighbour_slot)
        adjacent_sum = adjacent_total(block_shaped, ghost_faces, peclet_shaped).reshape(TOTAL_SLOTS, 3, BLOCK_EDGE ** 3)
        operator_result = viscosity[:, None, :] * (6.0 * present_iterate - adjacent_sum)
        return (right_hand_side - (present_iterate - prior_velocity) / STEP_DURATION - operator_result) * live_indicator[:, None, None]

    return lax.map(one_slice, (velocity_state, earlier, forcing_history))


def solve_frequency(pieces, viscosity, peclet_shaped, neighbour_holder, neighbour_slot):
    source_real, source_imag, shift_real, shift_imag = pieces
    diagonal = shift_real + 6.0 * viscosity[:, None, :]
    determinant = diagonal * diagonal + shift_imag * shift_imag
    real_component = jnp.zeros_like(source_real)
    imaginary_component = jnp.zeros_like(source_imag)
    for sweep_index in range(SWEEPS):
        stacked_slices = jnp.stack([real_component, imaginary_component], axis=1).reshape(TOTAL_SLOTS, 6, BLOCK_EDGE, BLOCK_EDGE, BLOCK_EDGE)
        ghost_faces = across_faces(stacked_slices, neighbour_holder, neighbour_slot)
        adjacent_sum = adjacent_total(stacked_slices, ghost_faces, peclet_shaped).reshape(TOTAL_SLOTS, 2, 3, BLOCK_EDGE ** 3)
        total_real = source_real + viscosity[:, None, :] * adjacent_sum[:, 0]
        total_imag = source_imag + viscosity[:, None, :] * adjacent_sum[:, 1]
        real_component = (diagonal * total_real + shift_imag * total_imag) / determinant
        imaginary_component = (diagonal * total_imag - shift_imag * total_real) / determinant
    return real_component, imaginary_component


def reference(iterate, forcing, initial_velocity, viscosity, peclet, live_patch_mask, neighbour_holder, neighbour_slot):
    velocity_state = jnp.transpose(iterate, (1, 0, 2, 3))
    forcing_history = jnp.transpose(forcing, (1, 0, 2, 3))
    live_indicator = live_patch_mask.astype(jnp.float32)
    peclet_shaped = peclet.reshape(TOTAL_SLOTS, 3, BLOCK_EDGE, BLOCK_EDGE, BLOCK_EDGE)
    residual_value = residual_grid(velocity_state, forcing_history, initial_velocity, viscosity, peclet_shaped, live_indicator, neighbour_holder, neighbour_slot)
    times = jnp.arange(WINDOW_SLICES, dtype=jnp.int32)
    product = (times[:, None] * times[None, :]) % WINDOW_SLICES
    angles = 2.0 * jnp.pi * product.astype(jnp.float32) / WINDOW_SLICES
    ramp = times.astype(jnp.float32) / WINDOW_SLICES
    twisted = jnp.power(ALPHA_SCALE, ramp)
    untwisted = jnp.power(ALPHA_SCALE, -ramp) / WINDOW_SLICES
    cosine = jnp.cos(angles)
    sine = jnp.sin(angles)
    source_real = jnp.einsum("kl,lncx->kncx", cosine * twisted[None, :], residual_value, precision=HIGHEST_PRECISION)
    source_imag = jnp.einsum("kl,lncx->kncx", -sine * twisted[None, :], residual_value, precision=HIGHEST_PRECISION)
    root = ALPHA_SCALE ** (1.0 / WINDOW_SLICES)
    base_angle = 2.0 * jnp.pi * times.astype(jnp.float32) / WINDOW_SLICES
    shift_real = (1.0 - root * jnp.cos(base_angle)) / STEP_DURATION
    shift_imag = root * jnp.sin(base_angle) / STEP_DURATION
    solver = partial(solve_frequency, viscosity=viscosity, peclet_shaped=peclet_shaped, neighbour_holder=neighbour_holder, neighbour_slot=neighbour_slot)
    real_component, imaginary_component = lax.map(solver, (source_real, source_imag, shift_real, shift_imag))
    update = jnp.einsum("lk,kncx->lncx", cosine * untwisted[:, None], real_component, precision=HIGHEST_PRECISION)
    update = update + jnp.einsum("lk,kncx->lncx", -sine * untwisted[:, None], imaginary_component, precision=HIGHEST_PRECISION)
    advanced_state = velocity_state + update
    corrected_residual = residual_grid(advanced_state, forcing_history, initial_velocity, viscosity, peclet_shaped, live_indicator, neighbour_holder, neighbour_slot)
    return jnp.transpose(advanced_state, (1, 0, 2, 3)), jnp.transpose(corrected_residual, (1, 0, 2, 3))
```

```python
import functools
import math

import jax
import jax.numpy as jnp
from jax import lax
from jax.experimental import pallas as pl
from jax.experimental.pallas import tpu as pltpu
from jax.sharding import PartitionSpec as P

WINDOW_SLICES = 16
BLOCK_EDGE = 16
SWEEPS = 5
STEP_DURATION = 0.5
ALPHA_SCALE = 0.1

ROWS = 32
LANES = 128
PAD = 8
TALL = ROWS + 2 * PAD
COMPONENTS = 3
GROUP = 16


def tables():
    n = WINDOW_SLICES
    root = ALPHA_SCALE ** (1.0 / n)
    forward, inverse, diagonals, coupling = [], [[] for _ in range(n)], [], []
    for mode in range(n // 2):
        angle = [2.0 * math.pi * (mode * time % n) / n for time in range(n)]
        alternate = [1.0 - 2.0 * (time % 2) for time in range(n)]
        twist = [root**time for time in range(n)]
        first = [math.cos(angle[t]) * twist[t] for t in range(n)]
        second = [(alternate[t] if mode == 0 else -math.sin(angle[t])) * twist[t] for t in range(n)]
        forward += [first, second]
        for t in range(n):
            back = root ** (-t) / n
            scale = 1.0 if mode == 0 else 2.0
            inverse[t] += [
                scale * math.cos(angle[t]) * back,
                (alternate[t] if mode == 0 else -2.0 * math.sin(angle[t])) * back,
            ]
        real = (1.0 - root * math.cos(2.0 * math.pi * mode / n)) / STEP_DURATION
        diagonals.append((real, (1.0 + root) / STEP_DURATION if mode == 0 else real))
        coupling.append(0.0 if mode == 0 else root * math.sin(2.0 * math.pi * mode / n) / STEP_DURATION)
    return forward, inverse, diagonals, coupling


def insert_bit(rank, dim, bit):
    low = 1 << dim
    return rank // low * (2 * low) + bit * low + rank % low


def remove_bit(slot, dim):
    low = 1 << dim
    return slot // (2 * low) * low + slot % low


def kernel(
    dims,
    weights,
    iterate,
    forcing,
    initial,
    viscosity,
    peclet,
    out_velocity,
    out_residual,
    state,
    residual,
    gathered,
    first_term,
    fields,
    factor_a,
    factor_b,
    spread,
    update,
    previous,
    res_send,
    res_recv,
    sweep_send,
    sweep_recv,
    send_sem,
    recv_sem,
    local_sem,
):
    time_devices, levels, slots, local = dims
    lead = slots // time_devices
    lead_bits = lead.bit_length() - 1
    forward, inverse, diagonals, coupling = tables()
    me = lax.axis_index("tm")
    place = lax.axis_index("space")
    place_bit = [place // (1 << b) % 2 for b in range(levels)]
    rows = lax.broadcasted_iota(jnp.int32, (ROWS, LANES), 0)
    lanes = lax.broadcasted_iota(jnp.int32, (ROWS, LANES), 1)
    odd_row = rows % 2 == 1
    z_index = lanes % BLOCK_EDGE
    y_block = lanes // BLOCK_EDGE

    space_links = []
    for b in range(levels):
        dim = b % 3
        if b + 3 < levels:
            side = 1 - (place_bit[b] + place_bit[b + 3]) % 2
        else:
            side = 1 - place_bit[b]
        partner = place + (1 << b) * (1 - 2 * place_bit[b])
        space_links.append((dim, side, {"space": partner}, 1 + b // 3))
    time_links = []
    for b in range(time_devices.bit_length() - 1):
        bit = me // (1 << b) % 2
        partner = me + (1 << b) * (1 - 2 * bit)
        time_links.append((lead_bits + b, 1 - bit, {"tm": partner}, 0))
    sweep_links = []
    for dim, side, partner, source in space_links:
        if dim >= lead_bits:
            step = 1 << (dim - lead_bits)
            partner = {**partner, "tm": me + step * (1 - 2 * (me // step % 2))}
        sweep_links.append((dim, side, partner, source))
    diagonal = [link[2] for link in sweep_links if len(link[2]) > 1]
    sweep_links += time_links

    barrier = pltpu.get_barrier_semaphore()
    greet = [link[2] for link in space_links]
    greet += diagonal
    greet += [{"tm": lax.rem(me + j, time_devices)} for j in range(1, time_devices)]
    for target in greet:
        pl.semaphore_signal(barrier, inc=1, device_id=target, device_id_type=pl.DeviceIdType.MESH)
    pl.semaphore_wait(barrier, len(greet))

    taken = [0]

    def send(source, target, device):
        number = taken[0]
        taken[0] += 1
        copy = pltpu.make_async_remote_copy(
            src_ref=source,
            dst_ref=target,
            send_sem=send_sem.at[number],
            recv_sem=recv_sem.at[number],
            device_id=device,
            device_id_type=pl.DeviceIdType.MESH,
        )
        copy.start()
        return copy

    def pack(load, count, dim, side, store):
        if dim == 0:
            def put(i, carry):
                store(pl.ds(PAD + 2 * i, 2), load(i, PAD + 30 * side, 2))
                return carry
            lax.fori_loop(0, count, put, 0)
            return

        def gather(i, packed):
            if dim == 1:
                parity = i // 8
                value = load(i, PAD + side - parity, ROWS)
                value = pltpu.roll(value, (i % 8 * BLOCK_EDGE + 128 - 112 * side) % 128, 1)
                chosen = (y_block == i % 8) & (rows % 2 == parity)
            else:
                value = load(i, PAD, ROWS)
                value = pltpu.roll(value, (i + 128 - 15 * side) % 128, 1)
                chosen = z_index == i
            return jnp.where(chosen, value, packed)

        packed = lax.fori_loop(0, count, gather, jnp.zeros((ROWS, LANES), jnp.float32))
        store(pl.ds(PAD, ROWS), packed)

    def received(load, i, dim, side):
        if dim == 0:
            return load(PAD + 2 * i, 2)
        if dim == 1:
            value = load(PAD + i // 8 - side, ROWS)
            return pltpu.roll(value, (112 * (1 - side) + 128 - i % 8 * BLOCK_EDGE) % 128, 1)
        return pltpu.roll(load(PAD, ROWS), (15 * side + 128 - i) % 128, 1)

    def beside(load, dim, side):
        if dim == 0:
            return load(PAD + 30 * (1 - side), 2)
        if dim == 1:
            return load(PAD + 1 - 2 * side, ROWS)
        return pltpu.roll(load(PAD, ROWS), (128 - 15 + 30 * side) % 128, 1)

    def adjacent(field, slot, coefficients, ghosts):
        upper, lower = [None] * 3, [None] * 3
        for dim, value, source in ghosts:
            high = weights[slot, dim, source, 1] * value
            low = weights[slot, dim, source, 0] * value
            upper[dim] = high if upper[dim] is None else upper[dim] + high
            lower[dim] = low if lower[dim] is None else lower[dim] + low
        field[pl.ds(PAD + ROWS, 2), :] = upper[0]
        field[pl.ds(PAD - 2, 2), :] = lower[0]
        value = field[pl.ds(PAD, ROWS), :]
        total = coefficients[0] * field[pl.ds(PAD + 2, ROWS), :]
        total = total + coefficients[1] * field[pl.ds(PAD - 2, ROWS), :]
        y_up = jnp.where(odd_row, upper[1], field[pl.ds(PAD + 1, ROWS), :])
        y_up = pltpu.roll(jnp.where(y_block == 0, y_up, value), 112, 1)
        y_low = jnp.where(odd_row, field[pl.ds(PAD - 1, ROWS), :], lower[1])
        y_low = pltpu.roll(jnp.where(y_block == 7, y_low, value), 16, 1)
        total = total + coefficients[2] * y_up + coefficients[3] * y_low
        z_up = jnp.where(z_index == 15, upper[2], pltpu.roll(value, 127, 1))
        z_low = jnp.where(z_index == 0, lower[2], pltpu.roll(value, 1, 1))
        return value, total + coefficients[4] * z_up + coefficients[5] * z_low

    def coefficients_of(slot):
        result = []
        for dim in range(3):
            number = peclet[slot, dim]
            result += [1.0 - number, 1.0 + number]
        return result

    def state_channel(i):
        return i // local, i % local

    def start_residual(phase):
        copies = []
        shift = send(
            state.at[:, :, local - 1, pl.ds(PAD, ROWS), :],
            previous.at[phase],
            {"tm": lax.rem(me + 1, time_devices)},
        )
        for number, (dim, side, partner, source) in enumerate(space_links):
            def one_slot(rank, carry, dim=dim, side=side, number=number):
                slot = insert_bit(rank, dim, side)

                def load(i, offset, size):
                    c, j = state_channel(i)
                    return state[c, slot, j, pl.ds(offset, size), :]

                def store(where, value):
                    res_send[phase, number, rank, where, :] = value

                pack(load, COMPONENTS * local, dim, side, store)
                return carry

            lax.fori_loop(0, slots // 2, one_slot, 0)
            copies.append(send(res_send.at[phase, number], res_recv.at[phase, number], partner))
        return shift, copies

    def residual_of(phase, c, store):
        def one_slot(slot, carry):
            coefficients = coefficients_of(slot)
            thickness = viscosity[slot]
            live = weights[slot, 0, 0, 2]
            bits = [slot // (1 << dim) % 2 for dim in range(3)]
            for j in range(local):
                i = c * local + j
                ghosts = []
                for dim in range(3):
                    other = slot + (1 << dim) * (1 - 2 * bits[dim])
                    load = lambda offset, size, other=other, j=j: state[
                        c, other, j, pl.ds(offset, size), :
                    ]
                    ghosts.append((dim, beside(load, dim, 1 - bits[dim]), 0))
                for number, (dim, side, partner, source) in enumerate(space_links):
                    rank = remove_bit(slot, dim)
                    load = lambda offset, size, number=number, rank=rank: res_recv[
                        phase, number, rank, pl.ds(offset, size), :
                    ]
                    ghosts.append((dim, received(load, i, dim, side), source))
                value, total = adjacent(state.at[c, slot, j], slot, coefficients, ghosts)
                if j == 0:
                    earlier = jnp.where(me == 0, initial[c, :, slot, :], previous[phase, c, slot])
                else:
                    earlier = state[c, slot, j - 1, pl.ds(PAD, ROWS), :]
                answer = forcing[slot, c, :, j, :] - (value - earlier) / STEP_DURATION
                answer = (answer - thickness * (6.0 * value - total)) * live
                store(slot, j, answer)
            return carry

        lax.fori_loop(0, slots, one_slot, 0)

    def take(slot, carry):
        for j in range(local):
            for c in range(COMPONENTS):
                state[c, slot, j, pl.ds(PAD, ROWS), :] = iterate[slot, c, :, j, :]
        return carry

    lax.fori_loop(0, slots, take, 0)
    shift, copies = start_residual(0)
    pending = [*copies]

    def make_factors(p, carry):
        slot = me * lead + p
        diffusion = 6.0 * viscosity[slot]
        for mode in range(GROUP // 2):
            real, second = diagonals[mode]
            if mode == 0:
                factor_a[p, mode] = 1.0 / (real + diffusion)
                factor_b[p, mode] = 1.0 / (second + diffusion)
            else:
                diagonal = real + diffusion
                determinant = diagonal * diagonal + coupling[mode] * coupling[mode]
                factor_a[p, mode] = diagonal / determinant
                factor_b[p, mode] = coupling[mode] / determinant
        return carry

    lax.fori_loop(0, lead, make_factors, 0)

    shift.wait()
    for copy in copies:
        copy.wait_recv()

    def exchange_time(source, target, number):
        moved = []
        for j in range(1, time_devices):
            peer = lax.rem(me + j, time_devices)
            moved.append(send(source(peer), target, {"tm": peer}))
        own = pltpu.make_async_copy(source(me), target, local_sem.at[number])
        own.start()
        return moved, own

    arrivals = []
    for c in range(COMPONENTS):
        def keep(slot, j, value, c=c):
            residual[c, slot, j] = value

        residual_of(0, c, keep)
        arrivals.append(
            exchange_time(
                lambda peer, c=c: residual.at[c, pl.ds(peer * lead, lead)], gathered.at[c, me], c
            )
        )

    def start_sweep(turn, c):
        copies = []
        for number, (dim, side, partner, source) in enumerate(sweep_links):
            inside = dim < lead_bits
            count = lead // 2 if inside else lead

            def one_slot(rank, carry, dim=dim, side=side, number=number, inside=inside):
                p = insert_bit(rank, dim, side) if inside else rank

                def load(i, offset, size):
                    return fields[turn % 2, c, p, i, pl.ds(offset, size), :]

                def store(where, value):
                    sweep_send[turn, c, number, rank, where, :] = value

                pack(load, GROUP, dim, side, store)
                return carry

            lax.fori_loop(0, count, one_slot, 0)
            copies.append(
                send(
                    sweep_send.at[turn, c, number, pl.ds(0, count)],
                    sweep_recv.at[turn, c, number, pl.ds(0, count)],
                    partner,
                )
            )
        pending.extend(copies)
        return copies

    sweeps = []
    for c in range(COMPONENTS):
        moved, own = arrivals[c]
        for copy in moved:
            copy.wait_recv()
        own.wait()
        pending.extend(moved)

        def transform(step, carry, c=c):
            p, chunk = step // (ROWS // 8), step % (ROWS // 8)
            at = pl.multiple_of(chunk * 8, 8)
            times = [
                gathered[c, t, p, j, pl.ds(at, 8), :] for t in range(time_devices) for j in range(local)
            ]
            for mode in range(GROUP // 2):
                sums = []
                for row in (forward[2 * mode], forward[2 * mode + 1]):
                    total = row[0] * times[0]
                    for t in range(1, WINDOW_SLICES):
                        if abs(row[t]) > 1e-12:
                            total = total + row[t] * times[t]
                    sums.append(total)
                a = factor_a[p, mode, pl.ds(at, 8), :]
                b = factor_b[p, mode, pl.ds(at, 8), :]
                if mode == 0:
                    real, imag = a * sums[0], b * sums[1]
                else:
                    real, imag = a * sums[0] + b * sums[1], a * sums[1] - b * sums[0]
                for part, value in ((0, real), (1, imag)):
                    first_term[c, p, 2 * mode + part, pl.ds(at, 8), :] = value
                    fields[0, c, p, 2 * mode + part, pl.ds(PAD + at, 8), :] = value
            return carry

        lax.fori_loop(0, lead * (ROWS // 8), transform, 0)
        sweeps.append(start_sweep(0, c))

    returns = []
    for turn in range(SWEEPS - 1):
        for c in range(COMPONENTS):
            for copy in sweeps[c]:
                copy.wait_recv()

            def one_slot(p, carry, turn=turn, c=c):
                slot = me * lead + p
                coefficients = coefficients_of(slot)
                thickness = viscosity[slot]

                def one_channel(i):
                    ghosts = []
                    for dim in range(lead_bits):
                        bit = p // (1 << dim) % 2
                        other = p + (1 << dim) * (1 - 2 * bit)
                        load = lambda offset, size, other=other: fields[
                            turn % 2, c, other, i, pl.ds(offset, size), :
                        ]
                        ghosts.append((dim, beside(load, dim, 1 - bit), 0))
                    for number, (dim, side, partner, source) in enumerate(sweep_links):
                        rank = remove_bit(p, dim) if dim < lead_bits else p
                        load = lambda offset, size, number=number, rank=rank: sweep_recv[
                            turn, c, number, rank, pl.ds(offset, size), :
                        ]
                        ghosts.append((dim, received(load, i, dim, side), source))
                    _, total = adjacent(fields.at[turn % 2, c, p, i], slot, coefficients, ghosts)
                    return thickness * total

                def one_mode(mode, carry):
                    real = one_channel(2 * mode)
                    imag = one_channel(2 * mode + 1)
                    a, b = factor_a[p, mode], factor_b[p, mode]
                    packed = mode == 0
                    cross = jnp.where(packed, 0.0, b)
                    imag_factor = jnp.where(packed, b, a)
                    new_real = first_term[c, p, 2 * mode] + (a * real + cross * imag)
                    new_imag = first_term[c, p, 2 * mode + 1] + (imag_factor * imag - cross * real)
                    later = (turn + 1) % 2
                    fields[later, c, p, 2 * mode, pl.ds(PAD, ROWS), :] = new_real
                    fields[later, c, p, 2 * mode + 1, pl.ds(PAD, ROWS), :] = new_imag
                    return carry

                return lax.fori_loop(0, GROUP // 2, one_mode, carry)

            lax.fori_loop(0, lead, one_slot, 0)
            if turn < SWEEPS - 2:
                sweeps[c] = start_sweep(turn + 1, c)
                continue

            def back(step, carry, c=c):
                p, chunk = step // (ROWS // 8), step % (ROWS // 8)
                at = pl.multiple_of(chunk * 8, 8)
                modes = [
                    fields[(SWEEPS - 1) % 2, c, p, i, pl.ds(PAD + at, 8), :] for i in range(GROUP)
                ]
                for time in range(WINDOW_SLICES):
                    row = inverse[time]
                    total = row[0] * modes[0]
                    for i in range(1, GROUP):
                        if abs(row[i]) > 1e-12:
                            total = total + row[i] * modes[i]
                    spread[c, time // local, p, time % local, pl.ds(at, 8), :] = total
                return carry

            lax.fori_loop(0, lead * (ROWS // 8), back, 0)
            returns.append(
                exchange_time(
                    lambda peer, c=c: spread.at[c, peer],
                    update.at[c, pl.ds(me * lead, lead)],
                    COMPONENTS + c,
                )
            )

    for c in range(COMPONENTS):
        moved, own = returns[c]
        for copy in moved:
            copy.wait_recv()
        own.wait()
        pending.extend(moved)

        def correct(slot, carry, c=c):
            for j in range(local):
                value = state[c, slot, j, pl.ds(PAD, ROWS), :] + update[c, slot, j]
                state[c, slot, j, pl.ds(PAD, ROWS), :] = value
                out_velocity[slot, c, :, j, :] = value
            return carry

        lax.fori_loop(0, slots, correct, 0)

    shift, copies = start_residual(1)
    pending.extend(copies)
    for copy in copies:
        copy.wait_recv()
    shift.wait()
    for c in range(COMPONENTS):
        def give(slot, j, value, c=c):
            out_residual[slot, c, :, j, :] = value

        residual_of(1, c, give)
    for copy in pending:
        copy.wait_send()


def body(
    iterate,
    forcing,
    initial_velocity,
    viscosity,
    peclet,
    live_patch_mask,
    neighbour_holder,
    neighbour_slot,
):
    time_devices = lax.axis_size("tm")
    levels = lax.axis_size("space").bit_length() - 1
    slots, local = iterate.shape[:2]
    lead = slots // time_devices
    place = lax.axis_index("space")

    holder = neighbour_holder.reshape(slots, 3, 2)
    depth = 1 + max(1, (levels + 2) // 3)
    sources = []
    for source in range(depth):
        per_dim = []
        for dim in range(3):
            b = dim + 3 * (source - 1)
            if source == 0:
                found = holder[:, dim] == place
            elif b < levels:
                found = holder[:, dim] == (place ^ (1 << b))
            else:
                found = jnp.zeros((slots, 2), bool)
            per_dim.append(found)
        sources.append(jnp.stack(per_dim, axis=1))
    weights = jnp.stack(sources, axis=2).astype(jnp.float32)
    live = jnp.broadcast_to(
        live_patch_mask.astype(jnp.float32)[:, None, None, None], (slots, 3, depth, 1)
    )
    weights = jnp.concatenate([weights, live], axis=3)

    def by_rows(array):
        split = array.reshape(array.shape[:-1] + (ROWS, LANES))
        return split.transpose((0, 2, 3, 1, 4) if split.ndim == 5 else (1, 2, 0, 3))

    def whole(array):
        return array.transpose(0, 3, 1, 2, 4).reshape(slots, local, COMPONENTS, ROWS * LANES)

    time_bits = time_devices.bit_length() - 1
    links = levels + time_bits
    turns = SWEEPS - 1
    copies = 2 * (1 + levels) + 2 * COMPONENTS * (time_devices - 1) + turns * COMPONENTS * links
    f32 = jnp.float32
    blocks = (ROWS, LANES)
    tall = (TALL, LANES)
    result = jax.ShapeDtypeStruct((slots, COMPONENTS, ROWS, local, LANES), f32)
    velocity, residual = pl.pallas_call(
        functools.partial(kernel, (time_devices, levels, slots, local)),
        out_shape=(result, result),
        in_specs=[pl.BlockSpec(memory_space=pltpu.SMEM)]
        + [pl.BlockSpec(memory_space=pltpu.VMEM)] * 5,
        out_specs=[pl.BlockSpec(memory_space=pltpu.VMEM)] * 2,
        scratch_shapes=[
            pltpu.VMEM((COMPONENTS, slots, local) + tall, f32),
            pltpu.VMEM((COMPONENTS, slots, local) + blocks, f32),
            pltpu.VMEM((COMPONENTS, time_devices, lead, local) + blocks, f32),
            pltpu.VMEM((COMPONENTS, lead, GROUP) + blocks, f32),
            pltpu.VMEM((2, COMPONENTS, lead, GROUP) + tall, f32),
            pltpu.VMEM((lead, GROUP // 2) + blocks, f32),
            pltpu.VMEM((lead, GROUP // 2) + blocks, f32),
            pltpu.VMEM((COMPONENTS, time_devices, lead, local) + blocks, f32),
            pltpu.VMEM((COMPONENTS, slots, local) + blocks, f32),
            pltpu.VMEM((2, COMPONENTS, slots) + blocks, f32),
            pltpu.VMEM((2, levels, slots // 2) + tall, f32),
            pltpu.VMEM((2, levels, slots // 2) + tall, f32),
            pltpu.VMEM((turns, COMPONENTS, links, lead) + tall, f32),
            pltpu.VMEM((turns, COMPONENTS, links, lead) + tall, f32),
            pltpu.SemaphoreType.DMA((copies,)),
            pltpu.SemaphoreType.DMA((copies,)),
            pltpu.SemaphoreType.DMA((2 * COMPONENTS,)),
        ],
        compiler_params=pltpu.CompilerParams(
            collective_id=0, has_side_effects=True, vmem_limit_bytes=60 * 1024 * 1024
        ),
    )(
        weights,
        by_rows(iterate),
        by_rows(forcing),
        by_rows(initial_velocity),
        viscosity.reshape((slots,) + blocks),
        peclet.reshape((slots, 3) + blocks),
    )
    return whole(velocity), whole(residual)


def solution(mesh):
    return jax.shard_map(
        body,
        mesh=mesh,
        in_specs=(
            P("space", "tm", None, None),
            P("space", "tm", None, None),
            P("space", None, None),
            P("space", None),
            P("space", None, None),
            P("space"),
            P("space", None),
            P("space", None),
        ),
        out_specs=(P("space", "tm", None, None), P("space", "tm", None, None)),
        check_vma=False,
    )
```

```python
import functools
import math

import jax
import jax.numpy as jnp
from jax import lax
from jax.experimental import pallas as pl
from jax.experimental.pallas import tpu as pltpu
from jax.sharding import PartitionSpec as P

WINDOW_SLICES = 16
BLOCK_EDGE = 16
SWEEPS = 5
STEP_DURATION = 0.5
ALPHA_SCALE = 0.1

ROWS = 32
LANES = 128
PAD = 8
TALL = ROWS + 2 * PAD
COMPONENTS = 3
GROUP = 16


def tables():
    n = WINDOW_SLICES
    root = ALPHA_SCALE ** (1.0 / n)
    forward, inverse, diagonals, coupling = [], [[] for _ in range(n)], [], []
    for mode in range(n // 2):
        angle = [2.0 * math.pi * (mode * time % n) / n for time in range(n)]
        alternate = [1.0 - 2.0 * (time % 2) for time in range(n)]
        twist = [root**time for time in range(n)]
        first = [math.cos(angle[t]) * twist[t] for t in range(n)]
        second = [(alternate[t] if mode == 0 else -math.sin(angle[t])) * twist[t] for t in range(n)]
        forward += [first, second]
        for t in range(n):
            back = root ** (-t) / n
            scale = 1.0 if mode == 0 else 2.0
            inverse[t] += [
                scale * math.cos(angle[t]) * back,
                (alternate[t] if mode == 0 else -2.0 * math.sin(angle[t])) * back,
            ]
        real = (1.0 - root * math.cos(2.0 * math.pi * mode / n)) / STEP_DURATION
        diagonals.append((real, (1.0 + root) / STEP_DURATION if mode == 0 else real))
        coupling.append(0.0 if mode == 0 else root * math.sin(2.0 * math.pi * mode / n) / STEP_DURATION)
    return forward, inverse, diagonals, coupling


def insert_bit(rank, dim, bit):
    low = 1 << dim
    return rank // low * (2 * low) + bit * low + rank % low


def remove_bit(slot, dim):
    low = 1 << dim
    return slot // (2 * low) * low + slot % low


def kernel(
    dims,
    weights,
    iterate,
    forcing,
    initial,
    viscosity,
    peclet,
    out_velocity,
    out_residual,
    state,
    residual,
    gathered,
    first_term,
    fields_even,
    fields_odd,
    factor_a,
    factor_b,
    spread,
    update,
    previous,
    res_send,
    res_recv,
    sweep_send,
    sweep_recv,
    send_sem,
    recv_sem,
    local_sem,
):
    time_devices, levels, slots, local = dims
    lead = slots // time_devices
    lead_bits = lead.bit_length() - 1
    fields = (fields_even, fields_odd)
    forward, inverse, diagonals, coupling = tables()
    me = lax.axis_index("tm")
    place = lax.axis_index("space")
    place_bit = [place // (1 << b) % 2 for b in range(levels)]
    rows = lax.broadcasted_iota(jnp.int32, (ROWS, LANES), 0)
    lanes = lax.broadcasted_iota(jnp.int32, (ROWS, LANES), 1)
    odd_row = rows % 2 == 1
    z_index = lanes % BLOCK_EDGE
    y_block = lanes // BLOCK_EDGE

    space_links = []
    for b in range(levels):
        dim = b % 3
        if b + 3 < levels:
            side = 1 - (place_bit[b] + place_bit[b + 3]) % 2
        else:
            side = 1 - place_bit[b]
        partner = place + (1 << b) * (1 - 2 * place_bit[b])
        space_links.append((dim, side, {"space": partner}, 1 + b // 3))
    time_links = []
    for b in range(time_devices.bit_length() - 1):
        bit = me // (1 << b) % 2
        partner = me + (1 << b) * (1 - 2 * bit)
        time_links.append((lead_bits + b, 1 - bit, {"tm": partner}, 0))
    sweep_links = []
    for dim, side, partner, source in space_links:
        if dim >= lead_bits:
            step = 1 << (dim - lead_bits)
            partner = {**partner, "tm": me + step * (1 - 2 * (me // step % 2))}
        sweep_links.append((dim, side, partner, source))
    diagonal = [link[2] for link in sweep_links if len(link[2]) > 1]
    sweep_links += time_links

    barrier = pltpu.get_barrier_semaphore()
    greet = [link[2] for link in space_links]
    greet += diagonal
    greet += [{"tm": lax.rem(me + j, time_devices)} for j in range(1, time_devices)]
    for target in greet:
        pl.semaphore_signal(barrier, inc=1, device_id=target, device_id_type=pl.DeviceIdType.MESH)
    pl.semaphore_wait(barrier, len(greet))

    taken = [0]

    def send(source, target, device):
        number = taken[0]
        taken[0] += 1
        copy = pltpu.make_async_remote_copy(
            src_ref=source,
            dst_ref=target,
            send_sem=send_sem.at[number],
            recv_sem=recv_sem.at[number],
            device_id=device,
            device_id_type=pl.DeviceIdType.MESH,
        )
        copy.start()
        return copy

    def pack(load, count, dim, side, store):
        if dim == 0:
            values = [load(i, PAD + 30 * side, 2) for i in range(count)]
            for i in range(count):
                store(pl.ds(PAD + 2 * i, 2), values[i])
            return
        packed = jnp.zeros((ROWS, LANES), jnp.float32)
        for i in range(count):
            if dim == 1:
                parity = i // 8
                value = load(i, PAD + side - parity, ROWS)
                value = pltpu.roll(value, (i % 8 * BLOCK_EDGE + 128 - 112 * side) % 128, 1)
                chosen = (y_block == i % 8) & (rows % 2 == parity)
            else:
                value = load(i, PAD, ROWS)
                value = pltpu.roll(value, (i + 128 - 15 * side) % 128, 1)
                chosen = z_index == i
            packed = jnp.where(chosen, value, packed)
        store(pl.ds(PAD, ROWS), packed)

    def received(load, i, dim, side):
        if dim == 0:
            return load(PAD + 2 * i, 2)
        if dim == 1:
            value = load(PAD + i // 8 - side, ROWS)
            return pltpu.roll(value, (112 * (1 - side) + 128 - i % 8 * BLOCK_EDGE) % 128, 1)
        return pltpu.roll(load(PAD, ROWS), (15 * side + 128 - i) % 128, 1)

    def beside(load, dim, side):
        if dim == 0:
            return load(PAD + 30 * (1 - side), 2)
        if dim == 1:
            return load(PAD + 1 - 2 * side, ROWS)
        return pltpu.roll(load(PAD, ROWS), (128 - 15 + 30 * side) % 128, 1)

    def source_weights(slot, sources):
        result = []
        for dim, source in sources:
            low, high = weights[slot, dim, source, 0], weights[slot, dim, source, 1]
            if dim == 0:
                result.append((low, high))
            else:
                upper = odd_row if dim == 1 else z_index == 15
                result.append(jnp.where(upper, high, low))
        return result

    def fill_ends(channels, ghosts_of, weighted):
        ends = []
        for i in range(len(channels)):
            low = high = None
            for value, (low_weight, high_weight) in zip(ghosts_of(i), weighted):
                low = low_weight * value if low is None else low + low_weight * value
                high = high_weight * value if high is None else high + high_weight * value
            ends.append((low, high))
        for field, (low, high) in zip(channels, ends):
            field[pl.ds(PAD - 2, 2), :] = low
            field[pl.ds(PAD + ROWS, 2), :] = high

    def adjacent(field, coefficients, ghosts):
        beyond = [None] * 3
        for dim, value, weight in ghosts:
            term = value * weight
            beyond[dim] = term if beyond[dim] is None else beyond[dim] + term
        value = field[pl.ds(PAD, ROWS), :]
        total = coefficients[0] * field[pl.ds(PAD + 2, ROWS), :]
        total = total + coefficients[1] * field[pl.ds(PAD - 2, ROWS), :]
        y_up = jnp.where(odd_row, beyond[1], field[pl.ds(PAD + 1, ROWS), :])
        y_up = pltpu.roll(jnp.where(y_block == 0, y_up, value), 112, 1)
        y_low = jnp.where(odd_row, field[pl.ds(PAD - 1, ROWS), :], beyond[1])
        y_low = pltpu.roll(jnp.where(y_block == 7, y_low, value), 16, 1)
        total = total + coefficients[2] * y_up + coefficients[3] * y_low
        z_up = jnp.where(z_index == 15, beyond[2], pltpu.roll(value, 127, 1))
        z_low = jnp.where(z_index == 0, beyond[2], pltpu.roll(value, 1, 1))
        return value, total + coefficients[4] * z_up + coefficients[5] * z_low

    def coefficients_of(slot):
        result = []
        for dim in range(3):
            number = peclet[slot, dim]
            result += [1.0 - number, 1.0 + number]
        return result

    def state_channel(i):
        return i // local, i % local

    def start_residual(phase):
        copies = []
        shift = send(
            state.at[:, :, local - 1, pl.ds(PAD, ROWS), :],
            previous.at[phase],
            {"tm": lax.rem(me + 1, time_devices)},
        )
        for number, (dim, side, partner, source) in enumerate(space_links):
            def one_slot(rank, carry, dim=dim, side=side, number=number):
                slot = insert_bit(rank, dim, side)

                def load(i, offset, size):
                    c, j = state_channel(i)
                    return state[c, slot, j, pl.ds(offset, size), :]

                def store(where, value):
                    res_send[phase, number, rank, where, :] = value

                pack(load, COMPONENTS * local, dim, side, store)
                return carry

            lax.fori_loop(0, slots // 2, one_slot, 0)
            copies.append(send(res_send.at[phase, number], res_recv.at[phase, number], partner))
        return shift, copies

    def residual_of(phase, c, store):
        def one_slot(slot, carry):
            coefficients = coefficients_of(slot)
            thickness = viscosity[slot]
            live = weights[slot, 0, 0, 2]
            bits = [slot // (1 << dim) % 2 for dim in range(3)]
            sources = [(dim, 0) for dim in range(3)]
            sources += [(dim, source) for dim, side, partner, source in space_links]
            weighted = source_weights(slot, sources)

            def ghosts_of(j, wanted):
                i = c * local + j
                found = []
                for dim in range(3):
                    if dim not in wanted:
                        continue
                    other = slot + (1 << dim) * (1 - 2 * bits[dim])
                    load = lambda offset, size: state[c, other, j, pl.ds(offset, size), :]
                    found.append((dim, beside(load, dim, 1 - bits[dim]), weighted[dim]))
                for number, (dim, side, partner, source) in enumerate(space_links):
                    if dim not in wanted:
                        continue
                    rank = remove_bit(slot, dim)
                    load = lambda offset, size: res_recv[
                        phase, number, rank, pl.ds(offset, size), :
                    ]
                    found.append((dim, received(load, i, dim, side), weighted[3 + number]))
                return found

            fill_ends(
                [state.at[c, slot, j] for j in range(local)],
                lambda j: [value for _, value, _ in ghosts_of(j, (0,))],
                [w for (dim, _), w in zip(sources, weighted) if dim == 0],
            )
            for j in range(local):
                value, total = adjacent(state.at[c, slot, j], coefficients, ghosts_of(j, (1, 2)))
                if j == 0:
                    earlier = jnp.where(me == 0, initial[c, :, slot, :], previous[phase, c, slot])
                else:
                    earlier = state[c, slot, j - 1, pl.ds(PAD, ROWS), :]
                answer = forcing[slot, c, :, j, :] - (value - earlier) / STEP_DURATION
                answer = (answer - thickness * (6.0 * value - total)) * live
                store(slot, j, answer)
            return carry

        lax.fori_loop(0, slots, one_slot, 0)

    def take(slot, carry):
        for j in range(local):
            for c in range(COMPONENTS):
                state[c, slot, j, pl.ds(PAD, ROWS), :] = iterate[slot, c, :, j, :]
        return carry

    lax.fori_loop(0, slots, take, 0)
    shift, copies = start_residual(0)
    pending = [*copies]

    def make_factors(p, carry):
        slot = me * lead + p
        diffusion = 6.0 * viscosity[slot]
        for mode in range(GROUP // 2):
            real, second = diagonals[mode]
            if mode == 0:
                factor_a[p, mode] = 1.0 / (real + diffusion)
                factor_b[p, mode] = 1.0 / (second + diffusion)
            else:
                diagonal = real + diffusion
                determinant = diagonal * diagonal + coupling[mode] * coupling[mode]
                factor_a[p, mode] = diagonal / determinant
                factor_b[p, mode] = coupling[mode] / determinant
        return carry

    lax.fori_loop(0, lead, make_factors, 0)

    shift.wait()
    for copy in copies:
        copy.wait_recv()

    def exchange_time(source, target, number):
        moved = []
        for j in range(1, time_devices):
            peer = lax.rem(me + j, time_devices)
            moved.append(send(source(peer), target, {"tm": peer}))
        own = pltpu.make_async_copy(source(me), target, local_sem.at[number])
        own.start()
        return moved, own

    arrivals = []
    for c in range(COMPONENTS):
        def keep(slot, j, value, c=c):
            residual[c, slot, j] = value

        residual_of(0, c, keep)
        arrivals.append(
            exchange_time(
                lambda peer, c=c: residual.at[c, pl.ds(peer * lead, lead)], gathered.at[c, me], c
            )
        )

    def start_sweep(turn, c):
        copies = []
        for number, (dim, side, partner, source) in enumerate(sweep_links):
            inside = dim < lead_bits
            count = lead // 2 if inside else lead

            def one_slot(rank, carry, dim=dim, side=side, number=number, inside=inside):
                p = insert_bit(rank, dim, side) if inside else rank

                def load(i, offset, size):
                    return fields[turn % 2][c, p, i, pl.ds(offset, size), :]

                def store(where, value):
                    sweep_send[turn, c, number, rank, where, :] = value

                pack(load, GROUP, dim, side, store)
                return carry

            lax.fori_loop(0, count, one_slot, 0)
            copies.append(
                send(
                    sweep_send.at[turn, c, number, pl.ds(0, count)],
                    sweep_recv.at[turn, c, number, pl.ds(0, count)],
                    partner,
                )
            )
        pending.extend(copies)
        return copies

    sweeps = []
    for c in range(COMPONENTS):
        moved, own = arrivals[c]
        for copy in moved:
            copy.wait_recv()
        own.wait()
        pending.extend(moved)

        def transform(step, carry, c=c):
            p, chunk = step // (ROWS // 8), step % (ROWS // 8)
            at = pl.multiple_of(chunk * 8, 8)
            times = [
                gathered[c, t, p, j, pl.ds(at, 8), :] for t in range(time_devices) for j in range(local)
            ]
            for mode in range(GROUP // 2):
                sums = []
                for row in (forward[2 * mode], forward[2 * mode + 1]):
                    total = row[0] * times[0]
                    for t in range(1, WINDOW_SLICES):
                        if abs(row[t]) > 1e-12:
                            total = total + row[t] * times[t]
                    sums.append(total)
                a = factor_a[p, mode, pl.ds(at, 8), :]
                b = factor_b[p, mode, pl.ds(at, 8), :]
                if mode == 0:
                    real, imag = a * sums[0], b * sums[1]
                else:
                    real, imag = a * sums[0] + b * sums[1], a * sums[1] - b * sums[0]
                for part, value in ((0, real), (1, imag)):
                    first_term[c, p, 2 * mode + part, pl.ds(at, 8), :] = value
                    fields_even[c, p, 2 * mode + part, pl.ds(PAD + at, 8), :] = value
            return carry

        lax.fori_loop(0, lead * (ROWS // 8), transform, 0)
        sweeps.append(start_sweep(0, c))

    returns = []
    for turn in range(SWEEPS - 1):
        for c in range(COMPONENTS):
            for copy in sweeps[c]:
                copy.wait_recv()

            def one_slot(p, carry, turn=turn, c=c):
                slot = me * lead + p
                coefficients = coefficients_of(slot)
                thickness = viscosity[slot]

                now, after = fields[turn % 2], fields[(turn + 1) % 2]
                sources = [(dim, 0) for dim in range(lead_bits)]
                sources += [(dim, source) for dim, side, partner, source in sweep_links]
                weighted = source_weights(slot, sources)

                def ghosts_of(i, wanted):
                    found = []
                    for dim in range(lead_bits):
                        if dim not in wanted:
                            continue
                        bit = p // (1 << dim) % 2
                        other = p + (1 << dim) * (1 - 2 * bit)
                        load = lambda offset, size: now[c, other, i, pl.ds(offset, size), :]
                        found.append((dim, beside(load, dim, 1 - bit), weighted[dim]))
                    for number, (dim, side, partner, source) in enumerate(sweep_links):
                        if dim not in wanted:
                            continue
                        rank = remove_bit(p, dim) if dim < lead_bits else p
                        load = lambda offset, size: sweep_recv[
                            turn, c, number, rank, pl.ds(offset, size), :
                        ]
                        found.append((dim, received(load, i, dim, side), weighted[lead_bits + number]))
                    return found

                fill_ends(
                    [now.at[c, p, i] for i in range(GROUP)],
                    lambda i: [value for _, value, _ in ghosts_of(i, (0,))],
                    [w for (dim, _), w in zip(sources, weighted) if dim == 0],
                )

                def one_channel(i):
                    _, total = adjacent(now.at[c, p, i], coefficients, ghosts_of(i, (1, 2)))
                    return thickness * total

                for mode in range(GROUP // 2):
                    real = one_channel(2 * mode)
                    imag = one_channel(2 * mode + 1)
                    a, b = factor_a[p, mode], factor_b[p, mode]
                    if mode == 0:
                        real, imag = a * real, b * imag
                    else:
                        real, imag = a * real + b * imag, a * imag - b * real
                    for part, change in ((0, real), (1, imag)):
                        after[c, p, 2 * mode + part, pl.ds(PAD, ROWS), :] = (
                            first_term[c, p, 2 * mode + part] + change
                        )
                return carry

            lax.fori_loop(0, lead, one_slot, 0)
            if turn < SWEEPS - 2:
                sweeps[c] = start_sweep(turn + 1, c)
                continue

            def back(step, carry, c=c):
                p, chunk = step // (ROWS // 8), step % (ROWS // 8)
                at = pl.multiple_of(chunk * 8, 8)
                modes = [
                    fields[(SWEEPS - 1) % 2][c, p, i, pl.ds(PAD + at, 8), :] for i in range(GROUP)
                ]
                for time in range(WINDOW_SLICES):
                    row = inverse[time]
                    total = row[0] * modes[0]
                    for i in range(1, GROUP):
                        if abs(row[i]) > 1e-12:
                            total = total + row[i] * modes[i]
                    spread[c, time // local, p, time % local, pl.ds(at, 8), :] = total
                return carry

            lax.fori_loop(0, lead * (ROWS // 8), back, 0)
            returns.append(
                exchange_time(
                    lambda peer, c=c: spread.at[c, peer],
                    update.at[c, pl.ds(me * lead, lead)],
                    COMPONENTS + c,
                )
            )

    for c in range(COMPONENTS):
        moved, own = returns[c]
        for copy in moved:
            copy.wait_recv()
        own.wait()
        pending.extend(moved)

        def correct(slot, carry, c=c):
            for j in range(local):
                value = state[c, slot, j, pl.ds(PAD, ROWS), :] + update[c, slot, j]
                state[c, slot, j, pl.ds(PAD, ROWS), :] = value
                out_velocity[slot, c, :, j, :] = value
            return carry

        lax.fori_loop(0, slots, correct, 0)

    shift, copies = start_residual(1)
    pending.extend(copies)
    for copy in copies:
        copy.wait_recv()
    shift.wait()
    for c in range(COMPONENTS):
        def give(slot, j, value, c=c):
            out_residual[slot, c, :, j, :] = value

        residual_of(1, c, give)
    for copy in pending:
        copy.wait_send()


def body(
    iterate,
    forcing,
    initial_velocity,
    viscosity,
    peclet,
    live_patch_mask,
    neighbour_holder,
    neighbour_slot,
):
    time_devices = lax.axis_size("tm")
    levels = lax.axis_size("space").bit_length() - 1
    slots, local = iterate.shape[:2]
    lead = slots // time_devices
    place = lax.axis_index("space")

    holder = neighbour_holder.reshape(slots, 3, 2)
    depth = 1 + max(1, (levels + 2) // 3)
    sources = []
    for source in range(depth):
        per_dim = []
        for dim in range(3):
            b = dim + 3 * (source - 1)
            if source == 0:
                found = holder[:, dim] == place
            elif b < levels:
                found = holder[:, dim] == (place ^ (1 << b))
            else:
                found = jnp.zeros((slots, 2), bool)
            per_dim.append(found)
        sources.append(jnp.stack(per_dim, axis=1))
    weights = jnp.stack(sources, axis=2).astype(jnp.float32)
    live = jnp.broadcast_to(
        live_patch_mask.astype(jnp.float32)[:, None, None, None], (slots, 3, depth, 1)
    )
    weights = jnp.concatenate([weights, live], axis=3)

    def by_rows(array):
        split = array.reshape(array.shape[:-1] + (ROWS, LANES))
        return split.transpose((0, 2, 3, 1, 4) if split.ndim == 5 else (1, 2, 0, 3))

    def whole(array):
        return array.transpose(0, 3, 1, 2, 4).reshape(slots, local, COMPONENTS, ROWS * LANES)

    time_bits = time_devices.bit_length() - 1
    links = levels + time_bits
    turns = SWEEPS - 1
    copies = 2 * (1 + levels) + 2 * COMPONENTS * (time_devices - 1) + turns * COMPONENTS * links
    f32 = jnp.float32
    blocks = (ROWS, LANES)
    tall = (TALL, LANES)
    result = jax.ShapeDtypeStruct((slots, COMPONENTS, ROWS, local, LANES), f32)
    velocity, residual = pl.pallas_call(
        functools.partial(kernel, (time_devices, levels, slots, local)),
        out_shape=(result, result),
        in_specs=[pl.BlockSpec(memory_space=pltpu.SMEM)]
        + [pl.BlockSpec(memory_space=pltpu.VMEM)] * 5,
        out_specs=[pl.BlockSpec(memory_space=pltpu.VMEM)] * 2,
        scratch_shapes=[
            pltpu.VMEM((COMPONENTS, slots, local) + tall, f32),
            pltpu.VMEM((COMPONENTS, slots, local) + blocks, f32),
            pltpu.VMEM((COMPONENTS, time_devices, lead, local) + blocks, f32),
            pltpu.VMEM((COMPONENTS, lead, GROUP) + blocks, f32),
            pltpu.VMEM((COMPONENTS, lead, GROUP) + tall, f32),
            pltpu.VMEM((COMPONENTS, lead, GROUP) + tall, f32),
            pltpu.VMEM((lead, GROUP // 2) + blocks, f32),
            pltpu.VMEM((lead, GROUP // 2) + blocks, f32),
            pltpu.VMEM((COMPONENTS, time_devices, lead, local) + blocks, f32),
            pltpu.VMEM((COMPONENTS, slots, local) + blocks, f32),
            pltpu.VMEM((2, COMPONENTS, slots) + blocks, f32),
            pltpu.VMEM((2, levels, slots // 2) + tall, f32),
            pltpu.VMEM((2, levels, slots // 2) + tall, f32),
            pltpu.VMEM((turns, COMPONENTS, links, lead) + tall, f32),
            pltpu.VMEM((turns, COMPONENTS, links, lead) + tall, f32),
            pltpu.SemaphoreType.DMA((copies,)),
            pltpu.SemaphoreType.DMA((copies,)),
            pltpu.SemaphoreType.DMA((2 * COMPONENTS,)),
        ],
        compiler_params=pltpu.CompilerParams(
            collective_id=0, has_side_effects=True, vmem_limit_bytes=60 * 1024 * 1024
        ),
    )(
        weights,
        by_rows(iterate),
        by_rows(forcing),
        by_rows(initial_velocity),
        viscosity.reshape((slots,) + blocks),
        peclet.reshape((slots, 3) + blocks),
    )
    return whole(velocity), whole(residual)


def solution(mesh):
    return jax.shard_map(
        body,
        mesh=mesh,
        in_specs=(
            P("space", "tm", None, None),
            P("space", "tm", None, None),
            P("space", None, None),
            P("space", None),
            P("space", None, None),
            P("space"),
            P("space", None),
            P("space", None),
        ),
        out_specs=(P("space", "tm", None, None), P("space", "tm", None, None)),
        check_vma=False,
    )
```
